32 devices in a mesh: batch: 8 (over z, y), mp: 4 (over x, core).
Axes of the slice: x: 2, y: 2, z: 4, core: 2. Of those that a mesh axis runs over, the one named last changes fastest.
Arguments:
- lookup_ids: int32 [64, 16384], P('batch'), may hold values from 0 to 8191
- table_feature: int32 [64], replicated, may hold values from 0 to 63, each once
- tables: bfloat16 [64, 8192, 128], P('batch'), may hold values from -6 to 6
- cross_down: bfloat16 [2, 8192, 512], P(None, 'mp'), may hold values from -0.0625 to 0.0625
- cross_up: bfloat16 [2, 512, 8192], P(None, None, 'mp'), may hold values from -0.25 to 0.25
- cross_bias: float32 [2, 8192], P(None, 'mp'), may hold values from -3 to 3
Outputs:
- crossed: bfloat16 [16384, 8192], P('batch', 'mp')
The draws below stay inside these ranges and needn't reach their ends.
Inputs may be any that keep to these rules, and one draw needn't show every extreme that they name: `table_feature`: each number appears once.
All inputs are finite; a program needn't handle non-finite values.
Results may differ from the reference program's by a relative error of at most 0.015.
Values may be sent and summed in bfloat16 or wider, within the bound.
No kernel may reach another device: no remote copies, remote signals or barrier semaphores. Data moves between devices by JAX's collectives and lax.ppermute only.
A program may use at most 128 MiB of HBM per device.

```python
import math
import jax
import jax.numpy as jnp
import numpy as np
from jax import lax

FEATS = 64
EMB = 128
RANK = 512
ROWS = 8192
LAYERS = 2
WIDTH = 8192
BATCH = 16384
N_MP = 4


def plant(drawn, stream_key, low, top_value):
    place = [jax.random.randint(jax.random.fold_in(stream_key, axis), (), 0, length) for axis, length in enumerate(drawn.shape)]
    main_axis = drawn.shape.index(max(drawn.shape))
    neighbour = place[:main_axis] + [(place[main_axis] + 1) % drawn.shape[main_axis]] + place[main_axis + 1:]
    return drawn.at[tuple(place)].set(low).at[tuple(neighbour)].set(top_value)


def shard_levels(own_key, dims, pieces, low, high):
    factor_of = 1.0
    for axis_at, blocks in pieces:
        draws = jax.random.uniform(jax.random.fold_in(jax.random.fold_in(own_key, 6), axis_at), (blocks,), jnp.float32, low / len(pieces), high / len(pieces))
        factor_of = factor_of * jnp.repeat(jnp.exp(draws), dims[axis_at] // blocks).reshape((-1,) + (1,) * (len(dims) - 1 - axis_at))
    return factor_of


def rank_table(number_of, slope):
    weights = [(1 << 20) // math.isqrt(rank ** slope) + 1 for rank in range(1, number_of + 1)]
    width = 1 + sum(weights) // (1 << 30)
    return np.cumsum(np.array([max(1, weight // width) for weight in weights]))


def skewed_ids(stream_key, shape, amount, slope):
    grid = rank_table(amount, slope)
    lot = jax.random.randint(jax.random.fold_in(stream_key, 1), shape, 0, int(grid[amount - 1]))
    standing = jnp.searchsorted(jnp.asarray(grid, jnp.int32), lot, side="right")
    return jax.random.permutation(jax.random.fold_in(stream_key, 2), amount)[standing].astype(jnp.int32)


def centred(key, extent, width, bound, cuts=(), held_as=jnp.bfloat16):
    values = jax.random.normal(key, extent, jnp.float32) * width
    if len(cuts) > 0:
        values = shard_levels(key, extent, cuts, -0.22, 0.18) * values
    return jnp.clip(values, min=-bound, max=bound).astype(held_as)


def setup_inputs(seed: int = 0) -> dict:
    streams_of = jax.random.split(jax.random.key(seed), 7)
    lookup_ids = plant(skewed_ids(streams_of[0], (FEATS, BATCH), ROWS, 2), jax.random.fold_in(streams_of[0], 3), 0, ROWS - 1).astype(jnp.int32)
    table_feature = jax.random.permutation(streams_of[1], FEATS).astype(jnp.int32)
    tables = centred(streams_of[2], (FEATS, ROWS, EMB), 1.0, 6.0, ((0, 8),))
    cross_down = centred(streams_of[3], (LAYERS, WIDTH, RANK), WIDTH ** -0.5, 0.0625, ((1, 4),))
    cross_up = centred(streams_of[4], (LAYERS, RANK, WIDTH), RANK ** -0.5, 0.25, ((2, 4),))
    cross_bias = centred(streams_of[5], (LAYERS, WIDTH), 0.5, 3.0, ((1, 4),), jnp.float32)
    return dict(lookup_ids=lookup_ids, table_feature=table_feature, tables=tables, cross_down=cross_down, cross_up=cross_up, cross_bias=cross_bias)


def reference(lookup_ids, table_feature, tables, cross_down, cross_up, cross_bias):
    looked = jax.vmap(lambda table, index: jnp.take(table, index, axis=0))(tables, lookup_ids)
    inverse = jnp.zeros((FEATS,), jnp.int32).at[table_feature].set(jnp.arange(FEATS, dtype=jnp.int32))
    by_feature = jnp.take(looked, inverse, axis=0)
    embedded = jnp.transpose(by_feature, (1, 2, 0)).reshape(BATCH, EMB * FEATS)
    block = WIDTH // N_MP
    state = embedded
    for layer in range(LAYERS):
        low_sum = jnp.zeros((BATCH, RANK), jnp.float32)
        for piece in range(N_MP):
            term = jnp.dot(state[:, piece * block:(piece + 1) * block], cross_down[layer, piece * block:(piece + 1) * block, :], preferred_element_type=jnp.float32)
            rounded = lax.optimization_barrier(term.astype(jnp.bfloat16))
            low_sum = low_sum + rounded.astype(jnp.float32)
        low = low_sum.astype(jnp.bfloat16)
        high = jnp.dot(low, cross_up[layer], preferred_element_type=jnp.float32) + cross_bias[layer][None, :]
        state = (embedded.astype(jnp.float32) * high + state.astype(jnp.float32)).astype(jnp.bfloat16)
    return state
```

```python
import functools

import jax
import jax.numpy as jnp
from jax import lax
from jax.experimental import pallas as pl
from jax.experimental.pallas import tpu as pltpu
from jax.sharding import PartitionSpec as P


PLAN = ((1, True), (2, True), (1, False))
UNROLL = 32
WIDEN = 1024
MIX = 32
MIB = 2**20


def gather_kernel(group_lanes, by_owner, place_ref, idx_ref, table_ref, *refs):
    outs, (wide, stage) = refs[:-2], refs[-2:]
    quads = stage.shape[0]
    turn = lax.rem(pl.program_id(0), quads)
    rows = wide.shape[0]
    count = stage.shape[1]
    widen_rows = min(WIDEN, rows)

    for t in range(quads):

        @pl.when(turn == t)
        def _():
            def widen(i, carry):
                at = pl.multiple_of(i * widen_rows, widen_rows)
                values = table_ref[0, pl.ds(at, widen_rows), :].astype(jnp.float32)
                if t:
                    values = pltpu.roll(values, t * group_lanes, 1)
                wide[pl.ds(at, widen_rows), :] = values
                return carry

            lax.fori_loop(0, rows // widen_rows, widen, 0)

    def fetch(i, carry):
        at = pl.multiple_of(i * UNROLL, UNROLL)
        for u in range(UNROLL):
            row = idx_ref[0, 0, at + u]
            stage[turn, pl.ds(at + u, 1), :] = wide[pl.ds(row, 1), :]
        return carry

    lax.fori_loop(0, count // UNROLL, fetch, 0)

    @pl.when(turn == quads - 1)
    def _():
        group = lax.broadcasted_iota(jnp.int32, (MIX, wide.shape[1]), 1) // group_lanes
        masks = [group == lax.rem(place_ref[0] + u, quads) for u in range(quads)]

        def piece(j, at):
            value = stage[quads - 1, pl.ds(at, MIX), :]
            for t in range(quads - 1):
                value = jnp.where(
                    masks[(j + t) % quads], stage[t, pl.ds(at, MIX), :], value
                )
            return value

        if by_owner:
            share = count // len(outs)
            for k, out in enumerate(outs):

                def mix(i, carry):
                    at = pl.multiple_of(i * MIX, MIX)
                    for j in range(quads):
                        out[j, pl.ds(at, MIX), :] = piece(j, k * share + at).astype(out.dtype)
                    return carry

                lax.fori_loop(0, share // MIX, mix, 0)
        else:

            def mix(i, carry):
                at = pl.multiple_of(i * MIX, MIX)
                for j, out in enumerate(outs):
                    out[pl.ds(at, MIX), :] = piece(j, at).astype(out.dtype)
                return carry

            lax.fori_loop(0, count // MIX, mix, 0)


def gather(place, ids, tables, parts, by_owner):
    slots, rows, emb = tables.shape
    owners, part_rows = ids.shape[1:]
    count = owners * part_rows
    lanes = emb // parts
    width = slots * lanes
    if slots % parts or rows % 1024 or count % 1024 or emb % 128:
        looked = jnp.stack(
            [jnp.take(tables[s], ids[s].reshape(-1), axis=0) for s in range(slots)], axis=1
        ).reshape(count, slots, parts, lanes)
        looked = jnp.transpose(looked, (2, 0, 1, 3)).reshape(parts, count, width)
        looked = jnp.concatenate([looked, looked], axis=0)
        looked = lax.dynamic_slice_in_dim(looked, place[0], parts, 0)
        looked = looked.reshape(parts, owners, part_rows, width)
        if by_owner:
            return [looked[:, k] for k in range(owners)]
        return [looked[j] for j in range(parts)]
    if by_owner:
        shapes = [(parts, part_rows, width)] * owners
        out_specs = [
            pl.BlockSpec((parts, part_rows, emb), lambda s, p: (0, 0, s // parts))
            for _ in shapes
        ]
    else:
        shapes = [(count, width)] * parts
        out_specs = [pl.BlockSpec((count, emb), lambda s, p: (0, s // parts)) for _ in shapes]
    outs = pl.pallas_call(
        functools.partial(gather_kernel, lanes, by_owner),
        grid_spec=pltpu.PrefetchScalarGridSpec(
            num_scalar_prefetch=1,
            grid=(slots,),
            in_specs=[
                pl.BlockSpec((1, 1, count), lambda s, p: (s, 0, 0), memory_space=pltpu.SMEM),
                pl.BlockSpec((1, rows, emb), lambda s, p: (s, 0, 0)),
            ],
            out_specs=out_specs,
            scratch_shapes=[
                pltpu.VMEM((rows, emb), jnp.float32),
                pltpu.VMEM((parts, count, emb), jnp.float32),
            ],
        ),
        out_shape=[jax.ShapeDtypeStruct(shape, tables.dtype) for shape in shapes],
        compiler_params=pltpu.CompilerParams(vmem_limit_bytes=60 * MIB),
        cost_estimate=pl.CostEstimate(
            flops=20000000 * slots, bytes_accessed=slots * rows * emb * 2, transcendentals=0
        ),
        name="gather",
    )(place, ids.reshape(slots, 1, count), tables)
    if by_owner:
        return outs
    return [out.reshape(owners, part_rows, width) for out in outs]


def lane_slots(place, slots, parts, lanes):
    if slots % parts:
        return jnp.arange(slots, dtype=jnp.int32)
    spot = jnp.arange(slots, dtype=jnp.int32)
    return (spot // parts) * parts + (spot % parts - place + parts) % parts


def project_kernel(by_owner, tile, place_ref, weight_ref, *refs):
    pieces, (x_ref, term_ref) = refs[:-2], refs[-2:]
    if by_owner:
        groups, (owners, part_rows, width) = len(pieces), pieces[0].shape
    else:
        owners, (groups, part_rows, width) = len(pieces), pieces[0].shape
    for j in range(groups):
        source = lax.rem(place_ref[0] + groups - j, groups)
        at = pl.multiple_of(source * part_rows, part_rows)
        for k in range(owners):
            piece = pieces[j][k] if by_owner else pieces[k][j]
            x_ref[pl.ds(at, part_rows), k * width : (k + 1) * width] = piece

    def body(i, carry):
        at = pl.multiple_of(i * tile, tile)
        term_ref[pl.ds(at, tile), :] = jnp.dot(
            x_ref[pl.ds(at, tile), :], weight_ref[...], preferred_element_type=jnp.float32
        ).astype(term_ref.dtype)
        return carry

    lax.fori_loop(0, x_ref.shape[0] // tile, body, 0)


def project(place, pieces, weight, by_owner):
    if by_owner:
        groups, (owners, part_rows, width) = len(pieces), pieces[0].shape
    else:
        owners, (groups, part_rows, width) = len(pieces), pieces[0].shape
    rows, total = groups * part_rows, owners * width
    if width % 128:
        parts = [
            jnp.concatenate(
                [pieces[j][k] if by_owner else pieces[k][j] for k in range(owners)], axis=1
            )
            for j in range(groups)
        ]
        parts = parts[:1] + parts[:0:-1]
        x = jnp.stack(parts + parts)
        start = (groups - place[0]) % groups
        x = lax.dynamic_slice_in_dim(x, start, groups, 0).reshape(rows, total)
        term = jnp.dot(x, weight, preferred_element_type=jnp.float32)
        return x, term.astype(jnp.bfloat16)
    return pl.pallas_call(
        functools.partial(project_kernel, by_owner, min(256, rows)),
        in_specs=[pl.BlockSpec(memory_space=pltpu.SMEM)]
        + [pl.BlockSpec(memory_space=pltpu.VMEM)] * (len(pieces) + 1),
        out_specs=[pl.BlockSpec(memory_space=pltpu.VMEM)] * 2,
        out_shape=[
            jax.ShapeDtypeStruct((rows, total), weight.dtype),
            jax.ShapeDtypeStruct((rows, weight.shape[1]), weight.dtype),
        ],
        compiler_params=pltpu.CompilerParams(vmem_limit_bytes=60 * MIB),
        cost_estimate=pl.CostEstimate(
            flops=2 * rows * total * weight.shape[1],
            bytes_accessed=4 * rows * total,
            transcendentals=0,
        ),
        name="project",
    )(place, weight, *pieces)


def last_kernel(low_ref, up_ref, bias_ref, embedded_ref, state_ref, *refs):
    out_ref = refs[-1]
    high = jnp.dot(low_ref[0], up_ref[...], preferred_element_type=jnp.float32) + bias_ref[...]
    value = embedded_ref[0].astype(jnp.float32) * high + state_ref[0].astype(jnp.float32)
    out_ref[0] = value.astype(out_ref.dtype)


def last(low, up, bias, embedded, state, out, start, shape):
    groups, share, width = shape
    part_rows = low.shape[0] // groups
    rank = low.shape[1]
    tile = part_rows
    while start % tile or tile > 256:
        tile //= 2
    row_spec = lambda size: pl.BlockSpec((1, tile, size), lambda j, i: (j, i, 0))
    operands = [
        low.reshape(groups, part_rows, rank),
        up,
        bias[None, :],
        embedded.reshape(groups, part_rows, width),
        state.reshape(groups, part_rows, width),
    ]
    in_specs = [
        row_spec(rank),
        pl.BlockSpec((rank, width), lambda j, i: (0, 0)),
        pl.BlockSpec((1, width), lambda j, i: (0, 0)),
        row_spec(width),
        row_spec(width),
    ]
    aliases = {}
    if out is not None:
        aliases = {len(operands): 0}
        operands.append(out)
        in_specs.append(pl.BlockSpec(memory_space=pl.ANY))
    rows = groups * part_rows
    return pl.pallas_call(
        last_kernel,
        grid=(groups, part_rows // tile),
        in_specs=in_specs,
        out_specs=pl.BlockSpec((1, tile, width), lambda j, i: (j, start // tile + i, 0)),
        out_shape=jax.ShapeDtypeStruct(shape, jnp.bfloat16),
        input_output_aliases=aliases,
        compiler_params=pltpu.CompilerParams(vmem_limit_bytes=40 * MIB),
        cost_estimate=pl.CostEstimate(
            flops=2 * rows * width * rank, bytes_accessed=6 * rows * width, transcendentals=0
        ),
        name="last",
    )(*operands)


def cyclic(size, step):
    return [(i, (i + step) % size) for i in range(size)]


def sum_over(term, axis):
    size = lax.axis_size(axis)
    if size & (size - 1):
        return lax.psum(term, axis)
    step = 1
    while step < size:
        other = lax.ppermute(term, axis, [(i, i ^ step) for i in range(size)])
        term = (term.astype(jnp.float32) + other.astype(jnp.float32)).astype(term.dtype)
        step *= 2
    return term


def tie(value, others):
    return lax.optimization_barrier((value, others))


def per_device(lookup_ids, table_feature, tables, cross_down, cross_up, cross_bias):
    slots, _, emb = tables.shape
    feats = table_feature.shape[0]
    owners, groups = lax.axis_size("batch"), lax.axis_size("mp")
    owner, member = lax.axis_index("batch"), lax.axis_index("mp")
    examples = lookup_ids.shape[1] // owners
    share = examples // groups
    lanes = emb // groups
    width = feats * lanes
    place = member.astype(jnp.int32)[None]
    wanted = lookup_ids.reshape(slots, owners, groups, share)
    wanted = lax.dynamic_index_in_dim(wanted, member, 2, keepdims=False)
    wanted = lax.dynamic_slice_in_dim(
        jnp.concatenate([wanted, wanted], axis=1), owner, owners, 1
    )

    unit = share // sum(size for size, _ in PLAN)
    starts, sizes, at = [], [], 0
    for size, _ in PLAN:
        starts.append(at)
        sizes.append(size * unit)
        at += size * unit

    held = []
    for (size, owner_first), begin, rows in zip(PLAN, starts, sizes):
        part = wanted[:, :, begin : begin + rows]
        if held:
            part, _ = tie(part, held[-1][0])
        found = gather(place, part, tables, groups, owner_first)
        if owner_first:
            moved = [found[0]] + [
                lax.ppermute(found[k], "batch", cyclic(owners, k)) for k in range(1, owners)
            ]
        else:
            moved = [found[0]] + [
                lax.ppermute(found[j], "mp", cyclic(groups, j)) for j in range(1, groups)
            ]
        held.append((found, moved))

    table_feature, _ = tie(table_feature, held[-1][0])
    source = (owner + owners - jnp.arange(owners)) % owners
    order = lane_slots(member, slots, groups, lanes)
    feature = table_feature.reshape(owners, slots)[source][:, order]
    if slots % groups:
        column = jnp.arange(lanes)[None, None, :] * feats + feature[:, :, None]
    else:
        column = jnp.arange(lanes)[None, None, :] * feats + feature[:, :, None]
    column = column.reshape(width)
    placing = (column[:, None] == jnp.arange(width)[None, :]).astype(jnp.bfloat16)
    placing = lax.optimization_barrier(placing)
    down_first = jnp.dot(placing, cross_down[0], preferred_element_type=jnp.float32)
    down_first = lax.optimization_barrier(down_first.astype(jnp.bfloat16))

    out = None
    for (size, owner_first), begin, rows, (found, moved) in zip(PLAN, starts, sizes, held):
        if owner_first:
            sent = [jnp.stack([moved[k][j] for k in range(owners)]) for j in range(groups)]
            pieces = [sent[0]] + [
                lax.ppermute(sent[j], "mp", cyclic(groups, j)) for j in range(1, groups)
            ]
        else:
            sent = [jnp.stack([moved[j][k] for j in range(groups)]) for k in range(owners)]
            pieces = [sent[0]] + [
                lax.ppermute(sent[k], "batch", cyclic(owners, k)) for k in range(1, owners)
            ]
        x, term = project(place, pieces, down_first, owner_first)
        embedded = jnp.dot(x, placing, preferred_element_type=jnp.float32).astype(jnp.bfloat16)
        state = embedded
        layers = cross_down.shape[0]
        for layer in range(layers):
            if layer:
                term = jnp.dot(state, cross_down[layer], preferred_element_type=jnp.float32)
                term = term.astype(jnp.bfloat16)
            low = sum_over(term, "mp")
            if layer < layers - 1:
                high = (
                    jnp.dot(low, cross_up[layer], preferred_element_type=jnp.float32)
                    + cross_bias[layer][None, :]
                )
                state = (
                    embedded.astype(jnp.float32) * high + state.astype(jnp.float32)
                ).astype(jnp.bfloat16)
            else:
                out = last(
                    low,
                    cross_up[layer],
                    cross_bias[layer],
                    embedded,
                    state,
                    out,
                    begin,
                    (groups, share, width),
                )
    return out.reshape(examples, width)


def solution(mesh):
    return jax.shard_map(
        per_device,
        mesh=mesh,
        in_specs=(
            P("batch", None),
            P(),
            P("batch", None, None),
            P(None, "mp", None),
            P(None, None, "mp"),
            P(None, "mp"),
        ),
        out_specs=P("batch", "mp"),
        check_vma=False,
    )
```

```python
import functools

import jax
import jax.numpy as jnp
from jax import lax
from jax.experimental import pallas as pl
from jax.experimental.pallas import tpu as pltpu
from jax.sharding import PartitionSpec as P


PLAN = ((3, True), (3, False), (2, False))
UNROLL = 32
WIDEN = 1024
MIX = 32
MIB = 2**20


def gather_kernel(by_owner, place_ref, idx_ref, table_ref, *refs):
    outs, (wide, stage) = refs[:-2], refs[-2:]
    slots, count, emb = stage.shape
    turn = pl.program_id(0)
    rows = wide.shape[0]
    lanes = emb // slots
    halves = outs[0].shape[-1] // emb
    parts = slots // halves

    def widen(i, carry):
        at = pl.multiple_of(i * WIDEN, WIDEN)
        wide[pl.ds(at, WIDEN), :] = table_ref[0, pl.ds(at, WIDEN), :].astype(jnp.float32)
        return carry

    lax.fori_loop(0, rows // WIDEN, widen, 0)

    def fetch(i, carry):
        at = pl.multiple_of(i * UNROLL, UNROLL)
        for u in range(UNROLL):
            row = idx_ref[0, 0, at + u]
            stage[turn, pl.ds(at + u, 1), :] = wide[pl.ds(row, 1), :]
        return carry

    lax.fori_loop(0, count // UNROLL, fetch, 0)

    @pl.when(turn == slots - 1)
    def _():
        group = lax.broadcasted_iota(jnp.int32, (MIX, emb), 1) // lanes
        masks = [
            group == lax.rem(place_ref[0] * halves + u, slots) for u in range(slots)
        ]

        def mixed(at):
            turned = [stage[0, pl.ds(at, MIX), :]]
            for t in range(1, slots):
                turned.append(pltpu.roll(stage[t, pl.ds(at, MIX), :], t * lanes, 1))
            for j in range(parts):
                for h in range(halves):
                    value = turned[-1]
                    for t in range(slots - 1):
                        value = jnp.where(
                            masks[(j * halves + h + t) % slots], turned[t], value
                        )
                    yield j, slice(h * emb, (h + 1) * emb), value.astype(outs[0].dtype)

        if by_owner:
            share = count // len(outs)
            for k, out in enumerate(outs):

                def mix(i, carry):
                    at = pl.multiple_of(i * MIX, MIX)
                    for j, columns, value in mixed(k * share + at):
                        out[j, pl.ds(at, MIX), columns] = value
                    return carry

                lax.fori_loop(0, share // MIX, mix, 0)
        else:

            def mix(i, carry):
                at = pl.multiple_of(i * MIX, MIX)
                for j, columns, value in mixed(at):
                    outs[j][pl.ds(at, MIX), columns] = value
                return carry

            lax.fori_loop(0, count // MIX, mix, 0)


def halves_of(slots, parts, emb):
    if slots % parts or emb % 128 or emb % slots:
        return 0
    return slots // parts


def gather(place, ids, tables, parts, by_owner):
    slots, rows, emb = tables.shape
    owners, part_rows = ids.shape[1:]
    count = owners * part_rows
    lanes = emb // parts
    width = slots * lanes
    if not halves_of(slots, parts, emb):
        looked = jnp.stack(
            [jnp.take(tables[s], ids[s].reshape(-1), axis=0) for s in range(slots)], axis=1
        ).reshape(count, slots, parts, lanes)
        looked = jnp.transpose(looked, (2, 0, 1, 3)).reshape(parts, count, width)
        looked = jnp.concatenate([looked, looked], axis=0)
        looked = lax.dynamic_slice_in_dim(looked, place[0], parts, 0)
        looked = looked.reshape(parts, owners, part_rows, width)
        if by_owner:
            return [looked[:, k] for k in range(owners)]
        return [looked[j] for j in range(parts)]
    if by_owner:
        shapes = [(parts, part_rows, width)] * owners
        out_specs = [pl.BlockSpec(shape, lambda s, p: (0, 0, 0)) for shape in shapes]
    else:
        shapes = [(count, width)] * parts
        out_specs = [pl.BlockSpec(shape, lambda s, p: (0, 0)) for shape in shapes]
    outs = pl.pallas_call(
        functools.partial(gather_kernel, by_owner),
        grid_spec=pltpu.PrefetchScalarGridSpec(
            num_scalar_prefetch=1,
            grid=(slots,),
            in_specs=[
                pl.BlockSpec((1, 1, count), lambda s, p: (s, 0, 0), memory_space=pltpu.SMEM),
                pl.BlockSpec((1, rows, emb), lambda s, p: (s, 0, 0)),
            ],
            out_specs=out_specs,
            scratch_shapes=[
                pltpu.VMEM((rows, emb), jnp.float32),
                pltpu.VMEM((slots, count, emb), jnp.float32),
            ],
        ),
        out_shape=[jax.ShapeDtypeStruct(shape, tables.dtype) for shape in shapes],
        compiler_params=pltpu.CompilerParams(vmem_limit_bytes=60 * MIB),
        cost_estimate=pl.CostEstimate(
            flops=1000, bytes_accessed=slots * rows * emb * 2, transcendentals=0
        ),
        name="gather",
    )(place, ids.reshape(slots, 1, count), tables)
    if by_owner:
        return outs
    return [out.reshape(owners, part_rows, width) for out in outs]


def swap_kernel(count, *refs):
    for a, source in enumerate(refs[:count]):
        for b, target in enumerate(refs[count:]):
            target[a] = source[b]


def swap(arrays):
    inner, part_rows, width = arrays[0].shape
    count = len(arrays)
    if width % 128:
        return [jnp.stack([array[b] for array in arrays]) for b in range(inner)]
    spec = pl.BlockSpec(memory_space=pltpu.VMEM)
    return pl.pallas_call(
        functools.partial(swap_kernel, count),
        in_specs=[spec] * count,
        out_specs=[spec] * inner,
        out_shape=[jax.ShapeDtypeStruct((count, part_rows, width), arrays[0].dtype)] * inner,
        compiler_params=pltpu.CompilerParams(vmem_limit_bytes=60 * MIB),
        cost_estimate=pl.CostEstimate(
            flops=1000, bytes_accessed=4 * inner * count * part_rows * width, transcendentals=0
        ),
        name="swap",
    )(*arrays)


def project_kernel(by_owner, tile, place_ref, weight_ref, *refs):
    pieces, (x_ref, term_ref) = refs[:-2], refs[-2:]
    if by_owner:
        groups, (owners, part_rows, width) = len(pieces), pieces[0].shape
    else:
        owners, (groups, part_rows, width) = len(pieces), pieces[0].shape
    halves = x_ref.shape[0]
    wide = width // halves
    for j in range(groups):
        source = lax.rem(place_ref[0] + groups - j, groups)
        at = pl.multiple_of(source * part_rows, part_rows)
        for k in range(owners):
            piece = pieces[j][k] if by_owner else pieces[k][j]
            for h in range(halves):
                x_ref[h, pl.ds(at, part_rows), k * wide : (k + 1) * wide] = piece[
                    :, h * wide : (h + 1) * wide
                ]

    def body(i, carry):
        at = pl.multiple_of(i * tile, tile)
        total = jnp.zeros((tile, weight_ref.shape[2]), jnp.float32)
        for h in range(halves):
            total = total + jnp.dot(
                x_ref[h, pl.ds(at, tile), :], weight_ref[h], preferred_element_type=jnp.float32
            )
        term_ref[pl.ds(at, tile), :] = total.astype(term_ref.dtype)
        return carry

    lax.fori_loop(0, x_ref.shape[1] // tile, body, 0)


def project(place, pieces, weight, by_owner):
    if by_owner:
        groups, (owners, part_rows, width) = len(pieces), pieces[0].shape
    else:
        owners, (groups, part_rows, width) = len(pieces), pieces[0].shape
    halves, half_width, rank = weight.shape
    rows = groups * part_rows
    if width % 128:
        parts = [
            jnp.concatenate(
                [pieces[j][k] if by_owner else pieces[k][j] for k in range(owners)], axis=1
            )
            for j in range(groups)
        ]
        parts = parts[:1] + parts[:0:-1]
        x = jnp.stack(parts + parts)
        start = (groups - place[0]) % groups
        x = lax.dynamic_slice_in_dim(x, start, groups, 0).reshape(1, rows, half_width)
        term = jnp.dot(x[0], weight[0], preferred_element_type=jnp.float32)
        return x, term.astype(jnp.bfloat16)
    spec = pl.BlockSpec(memory_space=pltpu.VMEM)
    return pl.pallas_call(
        functools.partial(project_kernel, by_owner, min(256, rows)),
        in_specs=[pl.BlockSpec(memory_space=pltpu.SMEM)] + [spec] * (len(pieces) + 1),
        out_specs=[spec] * 2,
        out_shape=[
            jax.ShapeDtypeStruct((halves, rows, half_width), weight.dtype),
            jax.ShapeDtypeStruct((rows, rank), weight.dtype),
        ],
        compiler_params=pltpu.CompilerParams(vmem_limit_bytes=60 * MIB),
        cost_estimate=pl.CostEstimate(
            flops=1000,
            bytes_accessed=4 * rows * halves * half_width,
            transcendentals=0,
        ),
        name="project",
    )(place, weight, *pieces)


def arrange_kernel(x_ref, placing_ref, out_ref):
    out_ref[...] = jnp.dot(
        x_ref[0], placing_ref[0], preferred_element_type=jnp.float32
    ).astype(out_ref.dtype)


def arrange(x, placing):
    halves, rows, half_width = x.shape
    tile = 256
    if half_width % 128 or rows % tile:
        parts = [
            jnp.dot(x[h], placing[h], preferred_element_type=jnp.float32).astype(x.dtype)
            for h in range(halves)
        ]
        return jnp.concatenate(parts, axis=1)
    return pl.pallas_call(
        arrange_kernel,
        grid=(halves, rows // tile),
        in_specs=[
            pl.BlockSpec((1, tile, half_width), lambda h, i: (h, i, 0)),
            pl.BlockSpec((1, half_width, half_width), lambda h, i: (h, 0, 0)),
        ],
        out_specs=pl.BlockSpec((tile, half_width), lambda h, i: (i, h)),
        out_shape=jax.ShapeDtypeStruct((rows, halves * half_width), x.dtype),
        compiler_params=pltpu.CompilerParams(vmem_limit_bytes=60 * MIB),
        cost_estimate=pl.CostEstimate(
            flops=1000,
            bytes_accessed=4 * rows * halves * half_width,
            transcendentals=0,
        ),
        name="arrange",
    )(x, placing)


def last_kernel(low_ref, up_ref, bias_ref, embedded_ref, state_ref, *refs):
    out_ref = refs[-1]
    high = jnp.dot(low_ref[0], up_ref[...], preferred_element_type=jnp.float32) + bias_ref[...]
    value = embedded_ref[0].astype(jnp.float32) * high + state_ref[0].astype(jnp.float32)
    out_ref[0] = value.astype(out_ref.dtype)


def last(low, up, bias, embedded, state, start, shape, out):
    groups, _, width = shape
    part_rows = low.shape[0] // groups
    rank = low.shape[1]
    tile = part_rows
    while start % tile or tile > 256:
        tile //= 2
    row_spec = lambda size: pl.BlockSpec((1, tile, size), lambda j, i: (j, i, 0))
    operands = [
        low.reshape(groups, part_rows, rank),
        up,
        bias[None, :],
        embedded.reshape(groups, part_rows, width),
        state.reshape(groups, part_rows, width),
    ]
    in_specs = [
        row_spec(rank),
        pl.BlockSpec((rank, width), lambda j, i: (0, 0)),
        pl.BlockSpec((1, width), lambda j, i: (0, 0)),
        row_spec(width),
        row_spec(width),
    ]
    aliases = {}
    if out is not None:
        aliases = {len(operands): 0}
        operands.append(out)
        in_specs.append(pl.BlockSpec(memory_space=pl.ANY))
    rows = groups * part_rows
    return pl.pallas_call(
        last_kernel,
        grid=(groups, part_rows // tile),
        in_specs=in_specs,
        out_specs=pl.BlockSpec((1, tile, width), lambda j, i: (j, start // tile + i, 0)),
        out_shape=jax.ShapeDtypeStruct(shape, jnp.bfloat16),
        input_output_aliases=aliases,
        compiler_params=pltpu.CompilerParams(vmem_limit_bytes=60 * MIB),
        cost_estimate=pl.CostEstimate(
            flops=1000, bytes_accessed=6 * rows * width, transcendentals=0
        ),
        name="last",
    )(*operands)


def spread(arrays, axis):
    size = len(arrays)
    moved = [arrays[0]]
    for step in range(1, size):
        pairs = [(i, (i + step) % size) for i in range(size)]
        moved.append(lax.ppermute(arrays[step], axis, pairs))
    return moved


def trade(value, axis, step):
    size = lax.axis_size(axis)
    return lax.ppermute(value, axis, [(i, i ^ step) for i in range(size)])


def add(one, other):
    return (one.astype(jnp.float32) + other.astype(jnp.float32)).astype(one.dtype)


def sum_over(term, axis):
    size = lax.axis_size(axis)
    rows = term.shape[0]
    if size & (size - 1) or size < 2 or rows % 32:
        return lax.psum(term, axis)
    half = rows // 2
    odd = lax.axis_index(axis) % 2
    kept = lax.dynamic_slice_in_dim(term, odd * half, half)
    given = lax.dynamic_slice_in_dim(term, (1 - odd) * half, half)
    kept = add(kept, trade(given, axis, 1))
    step = 2
    while step < size:
        kept = add(kept, trade(kept, axis, step))
        step *= 2
    other = trade(kept, axis, 1)
    return jnp.where(
        odd == 0,
        jnp.concatenate([kept, other], axis=0),
        jnp.concatenate([other, kept], axis=0),
    )


def tie(value, others):
    return lax.optimization_barrier((value, others))


def stages(lookup_ids, table_feature, tables, cross_down, cross_up, cross_bias):
    slots, _, emb = tables.shape
    feats = table_feature.shape[0]
    owners, groups = lax.axis_size("batch"), lax.axis_size("mp")
    owner, member = lax.axis_index("batch"), lax.axis_index("mp")
    examples = lookup_ids.shape[1] // owners
    share = examples // groups
    lanes = emb // groups
    width = feats * lanes
    place = member.astype(jnp.int32)[None]
    wanted = lookup_ids.reshape(slots, owners, groups, share)
    wanted = lax.dynamic_index_in_dim(wanted, member, 2, keepdims=False)
    wanted = lax.dynamic_slice_in_dim(
        jnp.concatenate([wanted, wanted], axis=1), owner, owners, 1
    )

    unit = share // sum(size for size, _ in PLAN)
    starts, sizes, at = [], [], 0
    for size, _ in PLAN:
        starts.append(at)
        sizes.append(size * unit)
        at += size * unit

    held = []
    for (size, owner_first), begin, rows in zip(PLAN, starts, sizes):
        part = wanted[:, :, begin : begin + rows]
        if held:
            part, _ = tie(part, held[-1][0])
        found = gather(place, part, tables, groups, owner_first)
        if owner_first:
            moved = spread(found, "batch")
        else:
            moved = spread(found, "mp")
        held.append((found, moved))

    table_feature, _ = tie(table_feature, held[-1][0])
    halves = halves_of(slots, groups, emb) or 1
    step = lanes // halves
    source = (owner + owners - jnp.arange(owners)) % owners
    spot = jnp.arange(slots)[None, :]
    if halves_of(slots, groups, emb):
        spot = (spot + slots - member * halves - jnp.arange(halves)[:, None]) % slots
    feature = table_feature[source[None, :, None] * slots + spot[:, None, :]]
    column = feature[:, :, :, None] + jnp.arange(step) * feats
    column = column.reshape(halves, width // halves)
    placing = (column[:, :, None] == jnp.arange(width // halves)).astype(jnp.bfloat16)
    placing = lax.optimization_barrier(placing)
    down_first = jnp.einsum(
        "hcd,hdr->hcr",
        placing,
        cross_down[0].reshape(halves, width // halves, -1),
        preferred_element_type=jnp.float32,
    )
    down_first = lax.optimization_barrier(down_first.astype(jnp.bfloat16))

    pieces_of = {}
    previous = down_first
    for c in sorted(range(len(PLAN)), key=lambda c: (c != 1, c)):
        owner_first, moved = PLAN[c][1], held[c][1]
        moved, _ = tie(moved, previous)
        sent = swap(moved)
        previous = sent
        if owner_first:
            pieces_of[c] = spread(sent, "mp")
        else:
            pieces_of[c] = spread(sent, "batch")

    out = finish = None
    for c, ((size, owner_first), begin, rows) in enumerate(zip(PLAN, starts, sizes)):
        final = c == len(PLAN) - 1
        pieces, _ = tie(pieces_of[c], previous)
        x, term = project(place, pieces, down_first, owner_first)
        if final and finish is not None:
            out = finish(out)
            x, out = tie(x, out)
        embedded = arrange(x, placing)
        previous = embedded
        state = embedded
        layers = cross_down.shape[0]
        for layer in range(layers):
            if layer:
                term = jnp.dot(state, cross_down[layer], preferred_element_type=jnp.float32)
                term = term.astype(jnp.bfloat16)
                if c == len(PLAN) - 2:
                    previous = term
            low = sum_over(term, "mp")
            if layer < layers - 1:
                high = (
                    jnp.dot(low, cross_up[layer], preferred_element_type=jnp.float32)
                    + cross_bias[layer][None, :]
                )
                state = (
                    embedded.astype(jnp.float32) * high + state.astype(jnp.float32)
                ).astype(jnp.bfloat16)
            else:
                if finish is not None and not final:
                    out = finish(out)
                finish = functools.partial(
                    last,
                    low,
                    cross_up[layer],
                    cross_bias[layer],
                    embedded,
                    state,
                    begin,
                    (groups, share, width),
                )
    out = finish(out)
    return out.reshape(examples, width)


def solution(mesh):
    return jax.shard_map(
        stages,
        mesh=mesh,
        in_specs=(
            P("batch", None),
            P(),
            P("batch", None, None),
            P(None, "mp", None),
            P(None, None, "mp"),
            P(None, "mp"),
        ),
        out_specs=P("batch", "mp"),
        check_vma=False,
    )
```

```python
import functools

import jax
import jax.numpy as jnp
from jax import lax
from jax.experimental import pallas as pl
from jax.experimental.pallas import tpu as pltpu
from jax.sharding import PartitionSpec as P


PLAN = ((3, True), (3, False), (2, False))
UNROLL = 32
WIDEN = 1024
MIX = 32
MIB = 2**20


def gather_kernel(by_owner, place_ref, idx_ref, table_ref, *refs):
    outs, (wide, stage) = refs[:-2], refs[-2:]
    slots, count, emb = stage.shape
    turn = pl.program_id(0)
    rows = wide.shape[0]
    lanes = emb // slots
    halves = outs[0].shape[-1] // emb
    parts = slots // halves

    def widen(i, carry):
        at = pl.multiple_of(i * WIDEN, WIDEN)
        wide[pl.ds(at, WIDEN), :] = table_ref[0, pl.ds(at, WIDEN), :].astype(jnp.float32)
        return carry

    lax.fori_loop(0, rows // WIDEN, widen, 0)

    def fetch(i, carry):
        at = pl.multiple_of(i * UNROLL, UNROLL)
        for u in range(UNROLL):
            row = idx_ref[0, 0, at + u]
            stage[turn, pl.ds(at + u, 1), :] = wide[pl.ds(row, 1), :]
        return carry

    lax.fori_loop(0, count // UNROLL, fetch, 0)

    @pl.when(turn == slots - 1)
    def _():
        group = lax.broadcasted_iota(jnp.int32, (MIX, emb), 1) // lanes
        masks = [
            group == lax.rem(place_ref[0] * halves + u, slots) for u in range(slots)
        ]

        def mixed(at):
            turned = [stage[0, pl.ds(at, MIX), :]]
            for t in range(1, slots):
                turned.append(pltpu.roll(stage[t, pl.ds(at, MIX), :], t * lanes, 1))
            for j in range(parts):
                for h in range(halves):
                    value = turned[-1]
                    for t in range(slots - 1):
                        value = jnp.where(
                            masks[(j * halves + h + t) % slots], turned[t], value
                        )
                    yield j, slice(h * emb, (h + 1) * emb), value.astype(outs[0].dtype)

        if by_owner:
            share = count // len(outs)
            for k, out in enumerate(outs):

                def mix(i, carry):
                    at = pl.multiple_of(i * MIX, MIX)
                    for j, columns, value in mixed(k * share + at):
                        out[j, pl.ds(at, MIX), columns] = value
                    return carry

                lax.fori_loop(0, share // MIX, mix, 0)
        else:

            def mix(i, carry):
                at = pl.multiple_of(i * MIX, MIX)
                for j, columns, value in mixed(at):
                    outs[j][pl.ds(at, MIX), columns] = value
                return carry

            lax.fori_loop(0, count // MIX, mix, 0)


def halves_of(slots, parts, emb):
    if slots % parts or emb % 128 or emb % slots:
        return 0
    return slots // parts


def gather(place, ids, tables, parts, by_owner):
    slots, rows, emb = tables.shape
    owners, part_rows = ids.shape[1:]
    count = owners * part_rows
    lanes = emb // parts
    width = slots * lanes
    if not halves_of(slots, parts, emb):
        looked = jnp.stack(
            [jnp.take(tables[s], ids[s].reshape(-1), axis=0) for s in range(slots)], axis=1
        ).reshape(count, slots, parts, lanes)
        looked = jnp.transpose(looked, (2, 0, 1, 3)).reshape(parts, count, width)
        looked = jnp.concatenate([looked, looked], axis=0)
        looked = lax.dynamic_slice_in_dim(looked, place[0], parts, 0)
        looked = looked.reshape(parts, owners, part_rows, width)
        if by_owner:
            return [looked[:, k] for k in range(owners)]
        return [looked[j] for j in range(parts)]
    if by_owner:
        shapes = [(parts, part_rows, width)] * owners
        out_specs = [pl.BlockSpec(shape, lambda s, p: (0, 0, 0)) for shape in shapes]
    else:
        shapes = [(count, width)] * parts
        out_specs = [pl.BlockSpec(shape, lambda s, p: (0, 0)) for shape in shapes]
    outs = pl.pallas_call(
        functools.partial(gather_kernel, by_owner),
        grid_spec=pltpu.PrefetchScalarGridSpec(
            num_scalar_prefetch=1,
            grid=(slots,),
            in_specs=[
                pl.BlockSpec((1, 1, count), lambda s, p: (s, 0, 0), memory_space=pltpu.SMEM),
                pl.BlockSpec((1, rows, emb), lambda s, p: (s, 0, 0)),
            ],
            out_specs=out_specs,
            scratch_shapes=[
                pltpu.VMEM((rows, emb), jnp.float32),
                pltpu.VMEM((slots, count, emb), jnp.float32),
            ],
        ),
        out_shape=[jax.ShapeDtypeStruct(shape, tables.dtype) for shape in shapes],
        compiler_params=pltpu.CompilerParams(vmem_limit_bytes=60 * MIB),
        cost_estimate=pl.CostEstimate(
            flops=1000, bytes_accessed=slots * rows * emb * 2, transcendentals=0
        ),
        name="gather",
    )(place, ids.reshape(slots, 1, count), tables)
    if by_owner:
        return outs
    return [out.reshape(owners, part_rows, width) for out in outs]


def swap_kernel(count, *refs):
    for a, source in enumerate(refs[:count]):
        for b, target in enumerate(refs[count:]):
            target[a] = source[b]


def swap(arrays):
    inner, part_rows, width = arrays[0].shape
    count = len(arrays)
    if width % 128:
        return [jnp.stack([array[b] for array in arrays]) for b in range(inner)]
    spec = pl.BlockSpec(memory_space=pltpu.VMEM)
    return pl.pallas_call(
        functools.partial(swap_kernel, count),
        in_specs=[spec] * count,
        out_specs=[spec] * inner,
        out_shape=[jax.ShapeDtypeStruct((count, part_rows, width), arrays[0].dtype)] * inner,
        compiler_params=pltpu.CompilerParams(vmem_limit_bytes=60 * MIB),
        cost_estimate=pl.CostEstimate(
            flops=1000, bytes_accessed=4 * inner * count * part_rows * width, transcendentals=0
        ),
        name="swap",
    )(*arrays)


def project_kernel(by_owner, tile, place_ref, weight_ref, *refs):
    pieces, (x_ref, term_ref) = refs[:-2], refs[-2:]
    if by_owner:
        groups, (owners, part_rows, width) = len(pieces), pieces[0].shape
    else:
        owners, (groups, part_rows, width) = len(pieces), pieces[0].shape
    halves = x_ref.shape[0]
    wide = width // halves
    for j in range(groups):
        source = lax.rem(place_ref[0] + groups - j, groups)
        at = pl.multiple_of(source * part_rows, part_rows)
        for k in range(owners):
            piece = pieces[j][k] if by_owner else pieces[k][j]
            for h in range(halves):
                x_ref[h, pl.ds(at, part_rows), k * wide : (k + 1) * wide] = piece[
                    :, h * wide : (h + 1) * wide
                ]

    def body(i, carry):
        at = pl.multiple_of(i * tile, tile)
        total = jnp.zeros((tile, weight_ref.shape[2]), jnp.float32)
        for h in range(halves):
            total = total + jnp.dot(
                x_ref[h, pl.ds(at, tile), :], weight_ref[h], preferred_element_type=jnp.float32
            )
        term_ref[pl.ds(at, tile), :] = total.astype(term_ref.dtype)
        return carry

    lax.fori_loop(0, x_ref.shape[1] // tile, body, 0)


def project(place, pieces, weight, by_owner):
    if by_owner:
        groups, (owners, part_rows, width) = len(pieces), pieces[0].shape
    else:
        owners, (groups, part_rows, width) = len(pieces), pieces[0].shape
    halves, half_width, rank = weight.shape
    rows = groups * part_rows
    if width % 128:
        parts = [
            jnp.concatenate(
                [pieces[j][k] if by_owner else pieces[k][j] for k in range(owners)], axis=1
            )
            for j in range(groups)
        ]
        parts = parts[:1] + parts[:0:-1]
        x = jnp.stack(parts + parts)
        start = (groups - place[0]) % groups
        x = lax.dynamic_slice_in_dim(x, start, groups, 0).reshape(1, rows, half_width)
        term = jnp.dot(x[0], weight[0], preferred_element_type=jnp.float32)
        return x, term.astype(jnp.bfloat16)
    spec = pl.BlockSpec(memory_space=pltpu.VMEM)
    return pl.pallas_call(
        functools.partial(project_kernel, by_owner, min(256, rows)),
        in_specs=[pl.BlockSpec(memory_space=pltpu.SMEM)] + [spec] * (len(pieces) + 1),
        out_specs=[spec] * 2,
        out_shape=[
            jax.ShapeDtypeStruct((halves, rows, half_width), weight.dtype),
            jax.ShapeDtypeStruct((rows, rank), weight.dtype),
        ],
        compiler_params=pltpu.CompilerParams(vmem_limit_bytes=60 * MIB),
        cost_estimate=pl.CostEstimate(
            flops=1000,
            bytes_accessed=4 * rows * halves * half_width,
            transcendentals=0,
        ),
        name="project",
    )(place, weight, *pieces)


def arrange_kernel(x_ref, placing_ref, out_ref):
    out_ref[...] = jnp.dot(
        x_ref[0], placing_ref[0], preferred_element_type=jnp.float32
    ).astype(out_ref.dtype)


def arrange(x, placing):
    halves, rows, half_width = x.shape
    tile = 256
    if half_width % 128 or rows % tile:
        parts = [
            jnp.dot(x[h], placing[h], preferred_element_type=jnp.float32).astype(x.dtype)
            for h in range(halves)
        ]
        return jnp.concatenate(parts, axis=1)
    return pl.pallas_call(
        arrange_kernel,
        grid=(halves, rows // tile),
        in_specs=[
            pl.BlockSpec((1, tile, half_width), lambda h, i: (h, i, 0)),
            pl.BlockSpec((1, half_width, half_width), lambda h, i: (h, 0, 0)),
        ],
        out_specs=pl.BlockSpec((tile, half_width), lambda h, i: (i, h)),
        out_shape=jax.ShapeDtypeStruct((rows, halves * half_width), x.dtype),
        compiler_params=pltpu.CompilerParams(vmem_limit_bytes=40 * MIB),
        cost_estimate=pl.CostEstimate(
            flops=1000,
            bytes_accessed=4 * rows * halves * half_width,
            transcendentals=0,
        ),
        name="arrange",
    )(x, placing)


def last_kernel(low_ref, up_ref, bias_ref, embedded_ref, state_ref, *refs):
    out_ref = refs[-1]
    high = jnp.dot(low_ref[0], up_ref[...], preferred_element_type=jnp.float32) + bias_ref[...]
    value = embedded_ref[0].astype(jnp.float32) * high + state_ref[0].astype(jnp.float32)
    out_ref[0] = value.astype(out_ref.dtype)


def last(low, up, bias, embedded, state, start, shape, out):
    groups, _, width = shape
    part_rows = low.shape[0] // groups
    rank = low.shape[1]
    tile = part_rows
    while start % tile or tile > 256:
        tile //= 2
    row_spec = lambda size: pl.BlockSpec((1, tile, size), lambda j, i: (j, i, 0))
    operands = [
        low.reshape(groups, part_rows, rank),
        up,
        bias[None, :],
        embedded.reshape(groups, part_rows, width),
        state.reshape(groups, part_rows, width),
    ]
    in_specs = [
        row_spec(rank),
        pl.BlockSpec((rank, width), lambda j, i: (0, 0)),
        pl.BlockSpec((1, width), lambda j, i: (0, 0)),
        row_spec(width),
        row_spec(width),
    ]
    aliases = {}
    if out is not None:
        aliases = {len(operands): 0}
        operands.append(out)
        in_specs.append(pl.BlockSpec(memory_space=pl.ANY))
    rows = groups * part_rows
    return pl.pallas_call(
        last_kernel,
        grid=(groups, part_rows // tile),
        in_specs=in_specs,
        out_specs=pl.BlockSpec((1, tile, width), lambda j, i: (j, start // tile + i, 0)),
        out_shape=jax.ShapeDtypeStruct(shape, jnp.bfloat16),
        input_output_aliases=aliases,
        compiler_params=pltpu.CompilerParams(vmem_limit_bytes=40 * MIB),
        cost_estimate=pl.CostEstimate(
            flops=1000, bytes_accessed=6 * rows * width, transcendentals=0
        ),
        name="last",
    )(*operands)


def spread(arrays, axis):
    size = len(arrays)
    moved = {0: arrays[0]}
    for step in sorted(range(1, size), key=lambda step: abs(2 * step - size)):
        pairs = [(i, (i + step) % size) for i in range(size)]
        moved[step] = lax.ppermute(arrays[step], axis, pairs)
    return [moved[step] for step in range(size)]


def trade(value, axis, step):
    size = lax.axis_size(axis)
    return lax.ppermute(value, axis, [(i, i ^ step) for i in range(size)])


def add(one, other):
    return (one.astype(jnp.float32) + other.astype(jnp.float32)).astype(one.dtype)


def sum_over(term, axis):
    size = lax.axis_size(axis)
    rows = term.shape[0]
    if size & (size - 1) or size < 2 or rows % 32:
        return lax.psum(term, axis)
    half = rows // 2
    odd = lax.axis_index(axis) % 2
    kept = lax.dynamic_slice_in_dim(term, odd * half, half)
    given = lax.dynamic_slice_in_dim(term, (1 - odd) * half, half)
    kept = add(kept, trade(given, axis, 1))
    step = 2
    while step < size:
        kept = add(kept, trade(kept, axis, step))
        step *= 2
    other = trade(kept, axis, 1)
    return jnp.where(
        odd == 0,
        jnp.concatenate([kept, other], axis=0),
        jnp.concatenate([other, kept], axis=0),
    )


def tie(value, others):
    return lax.optimization_barrier((value, others))


def stages(lookup_ids, table_feature, tables, cross_down, cross_up, cross_bias):
    slots, _, emb = tables.shape
    feats = table_feature.shape[0]
    owners, groups = lax.axis_size("batch"), lax.axis_size("mp")
    owner, member = lax.axis_index("batch"), lax.axis_index("mp")
    examples = lookup_ids.shape[1] // owners
    share = examples // groups
    lanes = emb // groups
    width = feats * lanes
    place = member.astype(jnp.int32)[None]
    wanted = lookup_ids.reshape(slots, owners, groups, share)
    wanted = lax.dynamic_index_in_dim(wanted, member, 2, keepdims=False)
    wanted = lax.dynamic_slice_in_dim(
        jnp.concatenate([wanted, wanted], axis=1), owner, owners, 1
    )

    unit = share // sum(size for size, _ in PLAN)
    starts, sizes, at = [], [], 0
    for size, _ in PLAN:
        starts.append(at)
        sizes.append(size * unit)
        at += size * unit

    held = []
    for (size, owner_first), begin, rows in zip(PLAN, starts, sizes):
        part = wanted[:, :, begin : begin + rows]
        if held:
            part, _ = tie(part, held[-1][0])
        found = gather(place, part, tables, groups, owner_first)
        if owner_first:
            moved = spread(found, "batch")
        else:
            moved = spread(found, "mp")
        held.append((found, moved))

    table_feature, _ = tie(table_feature, held[-1][0])
    halves = halves_of(slots, groups, emb) or 1
    step = lanes // halves
    source = (owner + owners - jnp.arange(owners)) % owners
    spot = jnp.arange(slots)[None, :]
    if halves_of(slots, groups, emb):
        spot = (spot + slots - member * halves - jnp.arange(halves)[:, None]) % slots
    feature = table_feature[source[None, :, None] * slots + spot[:, None, :]]
    column = feature[:, :, :, None] + jnp.arange(step) * feats
    column = column.reshape(halves, width // halves)
    placing = (column[:, :, None] == jnp.arange(width // halves)).astype(jnp.bfloat16)
    placing = lax.optimization_barrier(placing)
    down_first = jnp.einsum(
        "hcd,hdr->hcr",
        placing,
        cross_down[0].reshape(halves, width // halves, -1),
        preferred_element_type=jnp.float32,
    )
    down_first = lax.optimization_barrier(down_first.astype(jnp.bfloat16))

    pieces_of = {}
    previous = down_first
    for c in sorted(range(len(PLAN)), key=lambda c: (c != 1, c)):
        owner_first, moved = PLAN[c][1], held[c][1]
        moved, _ = tie(moved, previous)
        sent = swap(moved)
        previous = sent
        if owner_first:
            pieces_of[c] = spread(sent, "mp")
        else:
            pieces_of[c] = spread(sent, "batch")

    out = finish = None
    for c, ((size, owner_first), begin, rows) in enumerate(zip(PLAN, starts, sizes)):
        final = c == len(PLAN) - 1
        pieces, _ = tie(pieces_of[c], previous)
        x, term = project(place, pieces, down_first, owner_first)
        if final and finish is not None:
            out = finish(out)
            x, out = tie(x, out)
        embedded = arrange(x, placing)
        previous = embedded
        state = embedded
        layers = cross_down.shape[0]
        for layer in range(layers):
            if layer:
                term = jnp.dot(state, cross_down[layer], preferred_element_type=jnp.float32)
                term = term.astype(jnp.bfloat16)
                if c == len(PLAN) - 2:
                    previous = term
            low = sum_over(term, "mp")
            if layer < layers - 1:
                high = (
                    jnp.dot(low, cross_up[layer], preferred_element_type=jnp.float32)
                    + cross_bias[layer][None, :]
                )
                state = (
                    embedded.astype(jnp.float32) * high + state.astype(jnp.float32)
                ).astype(jnp.bfloat16)
            else:
                if finish is not None and not final:
                    out = finish(out)
                finish = functools.partial(
                    last,
                    low,
                    cross_up[layer],
                    cross_bias[layer],
                    embedded,
                    state,
                    begin,
                    (groups, share, width),
                )
    out = finish(out)
    return out.reshape(examples, width)


def solution(mesh):
    return jax.shard_map(
        stages,
        mesh=mesh,
        in_specs=(
            P("batch", None),
            P(),
            P("batch", None, None),
            P(None, "mp", None),
            P(None, None, "mp"),
            P(None, "mp"),
        ),
        out_specs=P("batch", "mp"),
        check_vma=False,
    )
```

```python
import functools
import math

import jax
import jax.numpy as jnp
from jax import lax
from jax.experimental import pallas as pl
from jax.experimental.pallas import tpu as pltpu
from jax.sharding import PartitionSpec as P


PLAN = ((3, True), (2, False), (3, False))
UNROLL = 64
WIDEN = 1024
MIX = 32
MIB = 2**20


def gather_kernel(by_owner, place_ref, idx_ref, table_ref, *refs):
    outs, (wide, stage) = refs[:-2], refs[-2:]
    slots, count, emb = stage.shape
    turn = pl.program_id(0)
    rows = wide.shape[0]
    lanes = emb // slots
    halves = outs[0].shape[-1] // emb
    parts = slots // halves

    def widen(i, carry):
        at = pl.multiple_of(i * WIDEN, WIDEN)
        wide[pl.ds(at, WIDEN), :] = table_ref[0, pl.ds(at, WIDEN), :].astype(jnp.float32)
        return carry

    lax.fori_loop(0, rows // WIDEN, widen, 0)

    def fetch(i, carry):
        at = pl.multiple_of(i * UNROLL, UNROLL)
        for u in range(UNROLL):
            row = idx_ref[0, 0, at + u]
            stage[turn, pl.ds(at + u, 1), :] = wide[pl.ds(row, 1), :]
        return carry

    lax.fori_loop(0, count // UNROLL, fetch, 0)

    @pl.when(turn == slots - 1)
    def _():
        group = lax.broadcasted_iota(jnp.int32, (MIX, emb), 1) // lanes
        masks = [
            group == lax.rem(place_ref[0] * halves + u, slots) for u in range(slots)
        ]

        def mixed(at):
            turned = [stage[0, pl.ds(at, MIX), :]]
            for t in range(1, slots):
                turned.append(pltpu.roll(stage[t, pl.ds(at, MIX), :], t * lanes, 1))
            for j in range(parts):
                for h in range(halves):
                    value = turned[-1]
                    for t in range(slots - 1):
                        value = jnp.where(
                            masks[(j * halves + h + t) % slots], turned[t], value
                        )
                    yield j, slice(h * emb, (h + 1) * emb), value.astype(outs[0].dtype)

        if by_owner:
            share = count // len(outs)
            for k, out in enumerate(outs):

                def mix(i, carry):
                    at = pl.multiple_of(i * MIX, MIX)
                    for j, columns, value in mixed(k * share + at):
                        out[j, pl.ds(at, MIX), columns] = value
                    return carry

                lax.fori_loop(0, share // MIX, mix, 0)
        else:

            def mix(i, carry):
                at = pl.multiple_of(i * MIX, MIX)
                for j, columns, value in mixed(at):
                    outs[j][pl.ds(at, MIX), columns] = value
                return carry

            lax.fori_loop(0, count // MIX, mix, 0)


def halves_of(slots, parts, emb):
    if slots % parts or emb % 128 or emb % slots:
        return 0
    return slots // parts


def gather(place, ids, tables, parts, by_owner):
    slots, rows, emb = tables.shape
    owners, part_rows = ids.shape[1:]
    count = owners * part_rows
    lanes = emb // parts
    width = slots * lanes
    if not halves_of(slots, parts, emb):
        looked = jnp.stack(
            [jnp.take(tables[s], ids[s].reshape(-1), axis=0) for s in range(slots)], axis=1
        ).reshape(count, slots, parts, lanes)
        looked = jnp.transpose(looked, (2, 0, 1, 3)).reshape(parts, count, width)
        looked = jnp.concatenate([looked, looked], axis=0)
        looked = lax.dynamic_slice_in_dim(looked, place[0], parts, 0)
        looked = looked.reshape(parts, owners, part_rows, width)
        if by_owner:
            return [looked[:, k] for k in range(owners)]
        return [looked[j] for j in range(parts)]
    if by_owner:
        shapes = [(parts, part_rows, width)] * owners
        out_specs = [pl.BlockSpec(shape, lambda s, p: (0, 0, 0)) for shape in shapes]
    else:
        shapes = [(count, width)] * parts
        out_specs = [pl.BlockSpec(shape, lambda s, p: (0, 0)) for shape in shapes]
    outs = pl.pallas_call(
        functools.partial(gather_kernel, by_owner),
        grid_spec=pltpu.PrefetchScalarGridSpec(
            num_scalar_prefetch=1,
            grid=(slots,),
            in_specs=[
                pl.BlockSpec((1, 1, count), lambda s, p: (s, 0, 0), memory_space=pltpu.SMEM),
                pl.BlockSpec((1, rows, emb), lambda s, p: (s, 0, 0)),
            ],
            out_specs=out_specs,
            scratch_shapes=[
                pltpu.VMEM((rows, emb), jnp.float32),
                pltpu.VMEM((slots, count, emb), jnp.float32),
            ],
        ),
        out_shape=[jax.ShapeDtypeStruct(shape, tables.dtype) for shape in shapes],
        compiler_params=pltpu.CompilerParams(vmem_limit_bytes=60 * MIB),
        cost_estimate=pl.CostEstimate(
            flops=1000, bytes_accessed=slots * rows * emb * 2, transcendentals=0
        ),
        name="gather",
    )(place, ids.reshape(slots, 1, count), tables)
    if by_owner:
        return outs
    return [out.reshape(owners, part_rows, width) for out in outs]


def swap_kernel(count, *refs):
    for a, source in enumerate(refs[:count]):
        for b, target in enumerate(refs[count:]):
            target[a] = source[b]


def swap(arrays):
    inner, part_rows, width = arrays[0].shape
    count = len(arrays)
    if width % 128:
        return [jnp.stack([array[b] for array in arrays]) for b in range(inner)]
    spec = pl.BlockSpec(memory_space=pltpu.VMEM)
    return pl.pallas_call(
        functools.partial(swap_kernel, count),
        in_specs=[spec] * count,
        out_specs=[spec] * inner,
        out_shape=[jax.ShapeDtypeStruct((count, part_rows, width), arrays[0].dtype)] * inner,
        compiler_params=pltpu.CompilerParams(vmem_limit_bytes=60 * MIB),
        cost_estimate=pl.CostEstimate(
            flops=1000, bytes_accessed=4 * inner * count * part_rows * width, transcendentals=0
        ),
        name="swap",
    )(*arrays)


def project_kernel(by_owner, tile, place_ref, weight_ref, *refs):
    pieces, (x_ref, term_ref) = refs[:-2], refs[-2:]
    if by_owner:
        groups, (owners, part_rows, width) = len(pieces), pieces[0].shape
    else:
        owners, (groups, part_rows, width) = len(pieces), pieces[0].shape
    halves = x_ref.shape[0]
    wide = width // halves
    for j in range(groups):
        source = lax.rem(place_ref[0] + groups - j, groups)
        at = pl.multiple_of(source * part_rows, part_rows)
        for k in range(owners):
            piece = pieces[j][k] if by_owner else pieces[k][j]
            for h in range(halves):
                x_ref[h, pl.ds(at, part_rows), k * wide : (k + 1) * wide] = piece[
                    :, h * wide : (h + 1) * wide
                ]

    def body(i, carry):
        at = pl.multiple_of(i * tile, tile)
        total = jnp.zeros((tile, weight_ref.shape[2]), jnp.float32)
        for h in range(halves):
            total = total + jnp.dot(
                x_ref[h, pl.ds(at, tile), :], weight_ref[h], preferred_element_type=jnp.float32
            )
        term_ref[pl.ds(at, tile), :] = total.astype(term_ref.dtype)
        return carry

    lax.fori_loop(0, x_ref.shape[1] // tile, body, 0)


def project(place, pieces, weight, by_owner):
    if by_owner:
        groups, (owners, part_rows, width) = len(pieces), pieces[0].shape
    else:
        owners, (groups, part_rows, width) = len(pieces), pieces[0].shape
    halves, half_width, rank = weight.shape
    rows = groups * part_rows
    if width % 128:
        parts = [
            jnp.concatenate(
                [pieces[j][k] if by_owner else pieces[k][j] for k in range(owners)], axis=1
            )
            for j in range(groups)
        ]
        parts = parts[:1] + parts[:0:-1]
        x = jnp.stack(parts + parts)
        start = (groups - place[0]) % groups
        x = lax.dynamic_slice_in_dim(x, start, groups, 0).reshape(1, rows, half_width)
        term = jnp.dot(x[0], weight[0], preferred_element_type=jnp.float32)
        return x, term.astype(jnp.bfloat16)
    spec = pl.BlockSpec(memory_space=pltpu.VMEM)
    return pl.pallas_call(
        functools.partial(project_kernel, by_owner, min(256, rows)),
        in_specs=[pl.BlockSpec(memory_space=pltpu.SMEM)] + [spec] * (len(pieces) + 1),
        out_specs=[spec] * 2,
        out_shape=[
            jax.ShapeDtypeStruct((halves, rows, half_width), weight.dtype),
            jax.ShapeDtypeStruct((rows, rank), weight.dtype),
        ],
        compiler_params=pltpu.CompilerParams(vmem_limit_bytes=60 * MIB),
        cost_estimate=pl.CostEstimate(
            flops=1000,
            bytes_accessed=4 * rows * halves * half_width,
            transcendentals=0,
        ),
        name="project",
    )(place, weight, *pieces)


def arrange_kernel(x_ref, placing_ref, out_ref):
    out_ref[...] = jnp.dot(
        x_ref[0], placing_ref[0], preferred_element_type=jnp.float32
    ).astype(out_ref.dtype)


def arrange(x, placing):
    halves, rows, half_width = x.shape
    tile = 256
    if half_width % 128 or rows % tile:
        parts = [
            jnp.dot(x[h], placing[h], preferred_element_type=jnp.float32).astype(x.dtype)
            for h in range(halves)
        ]
        return jnp.concatenate(parts, axis=1)
    return pl.pallas_call(
        arrange_kernel,
        grid=(halves, rows // tile),
        in_specs=[
            pl.BlockSpec((1, tile, half_width), lambda h, i: (h, i, 0)),
            pl.BlockSpec((1, half_width, half_width), lambda h, i: (h, 0, 0)),
        ],
        out_specs=pl.BlockSpec((tile, half_width), lambda h, i: (i, h)),
        out_shape=jax.ShapeDtypeStruct((rows, halves * half_width), x.dtype),
        compiler_params=pltpu.CompilerParams(vmem_limit_bytes=40 * MIB),
        cost_estimate=pl.CostEstimate(
            flops=1000,
            bytes_accessed=4 * rows * halves * half_width,
            transcendentals=0,
        ),
        name="arrange",
    )(x, placing)


def last_kernel(low_ref, up_ref, bias_ref, embedded_ref, state_ref, *refs):
    out_ref = refs[-1]
    high = jnp.dot(low_ref[0], up_ref[...], preferred_element_type=jnp.float32) + bias_ref[...]
    value = embedded_ref[0].astype(jnp.float32) * high + state_ref[0].astype(jnp.float32)
    out_ref[0] = value.astype(out_ref.dtype)


def last(low, up, bias, embedded, state, start, shape, out):
    groups, _, width = shape
    part_rows = low.shape[0] // groups
    rank = low.shape[1]
    tile = math.gcd(part_rows, start)
    while tile > 256:
        tile //= 2
    row_spec = lambda size: pl.BlockSpec((1, tile, size), lambda j, i: (j, i, 0))
    operands = [
        low.reshape(groups, part_rows, rank),
        up,
        bias[None, :],
        embedded.reshape(groups, part_rows, width),
        state.reshape(groups, part_rows, width),
    ]
    in_specs = [
        row_spec(rank),
        pl.BlockSpec((rank, width), lambda j, i: (0, 0)),
        pl.BlockSpec((1, width), lambda j, i: (0, 0)),
        row_spec(width),
        row_spec(width),
    ]
    aliases = {}
    if out is not None:
        aliases = {len(operands): 0}
        operands.append(out)
        in_specs.append(pl.BlockSpec(memory_space=pl.ANY))
    rows = groups * part_rows
    return pl.pallas_call(
        last_kernel,
        grid=(groups, part_rows // tile),
        in_specs=in_specs,
        out_specs=pl.BlockSpec((1, tile, width), lambda j, i: (j, start // tile + i, 0)),
        out_shape=jax.ShapeDtypeStruct(shape, jnp.bfloat16),
        input_output_aliases=aliases,
        compiler_params=pltpu.CompilerParams(vmem_limit_bytes=40 * MIB),
        cost_estimate=pl.CostEstimate(
            flops=1000, bytes_accessed=6 * rows * width, transcendentals=0
        ),
        name="last",
    )(*operands)


def spread(arrays, axis):
    size = len(arrays)
    moved = {0: arrays[0]}
    for step in sorted(range(1, size), key=lambda step: abs(2 * step - size)):
        pairs = [(i, (i + step) % size) for i in range(size)]
        moved[step] = lax.ppermute(arrays[step], axis, pairs)
    return [moved[step] for step in range(size)]


def trade(value, axis, step):
    size = lax.axis_size(axis)
    return lax.ppermute(value, axis, [(i, i ^ step) for i in range(size)])


def add(one, other):
    return (one.astype(jnp.float32) + other.astype(jnp.float32)).astype(one.dtype)


def sum_over(term, axis):
    size = lax.axis_size(axis)
    rows = term.shape[0]
    if size & (size - 1) or size < 2 or rows % 32:
        return lax.psum(term, axis)
    half = rows // 2
    odd = lax.axis_index(axis) % 2
    kept = lax.dynamic_slice_in_dim(term, odd * half, half)
    given = lax.dynamic_slice_in_dim(term, (1 - odd) * half, half)
    kept = add(kept, trade(given, axis, 1))
    step = 2
    while step < size:
        kept = add(kept, trade(kept, axis, step))
        step *= 2
    other = trade(kept, axis, 1)
    return jnp.where(
        odd == 0,
        jnp.concatenate([kept, other], axis=0),
        jnp.concatenate([other, kept], axis=0),
    )


def tie(value, others):
    return lax.optimization_barrier((value, others))


def stages(lookup_ids, table_feature, tables, cross_down, cross_up, cross_bias):
    slots, _, emb = tables.shape
    feats = table_feature.shape[0]
    owners, groups = lax.axis_size("batch"), lax.axis_size("mp")
    owner, member = lax.axis_index("batch"), lax.axis_index("mp")
    examples = lookup_ids.shape[1] // owners
    share = examples // groups
    lanes = emb // groups
    width = feats * lanes
    place = member.astype(jnp.int32)[None]
    wanted = lookup_ids.reshape(slots, owners, groups, share)
    wanted = lax.dynamic_index_in_dim(wanted, member, 2, keepdims=False)
    wanted = lax.dynamic_slice_in_dim(
        jnp.concatenate([wanted, wanted], axis=1), owner, owners, 1
    )

    unit = share // sum(size for size, _ in PLAN)
    sizes = [size * unit for size, _ in PLAN]
    starts, at = [0] * len(PLAN), 0
    for c in sorted(range(len(PLAN)), key=lambda c: -sizes[c]):
        starts[c] = at
        at += sizes[c]

    held = []
    for (size, owner_first), begin, rows in zip(PLAN, starts, sizes):
        part = wanted[:, :, begin : begin + rows]
        if held:
            part, _ = tie(part, held[-1][0])
        found = gather(place, part, tables, groups, owner_first)
        if owner_first:
            moved = spread(found, "batch")
        else:
            moved = spread(found, "mp")
        held.append((found, moved))

    table_feature, _ = tie(table_feature, held[-1][0])
    halves = halves_of(slots, groups, emb) or 1
    step = lanes // halves
    source = (owner + owners - jnp.arange(owners)) % owners
    spot = jnp.arange(slots)[None, :]
    if halves_of(slots, groups, emb):
        spot = (spot + slots - member * halves - jnp.arange(halves)[:, None]) % slots
    feature = table_feature[source[None, :, None] * slots + spot[:, None, :]]
    column = feature[:, :, :, None] + jnp.arange(step) * feats
    column = column.reshape(halves, width // halves)
    placing = (column[:, :, None] == jnp.arange(width // halves)).astype(jnp.bfloat16)
    placing = lax.optimization_barrier(placing)
    down_first = jnp.einsum(
        "hcd,hdr->hcr",
        placing,
        cross_down[0].reshape(halves, width // halves, -1),
        preferred_element_type=jnp.float32,
    )
    down_first = lax.optimization_barrier(down_first.astype(jnp.bfloat16))

    pieces_of = {}
    previous = down_first
    for c in sorted(range(len(PLAN)), key=lambda c: (c != 1, c)):
        owner_first, moved = PLAN[c][1], held[c][1]
        moved, _ = tie(moved, previous)
        sent = swap(moved)
        previous = sent
        if owner_first:
            pieces_of[c] = spread(sent, "mp")
        else:
            pieces_of[c] = spread(sent, "batch")

    out = finish = None
    for c, ((size, owner_first), begin, rows) in enumerate(zip(PLAN, starts, sizes)):
        final = c == len(PLAN) - 1
        pieces, _ = tie(pieces_of[c], previous)
        x, term = project(place, pieces, down_first, owner_first)
        if final and finish is not None:
            out = finish(out)
            x, out = tie(x, out)
        embedded = arrange(x, placing)
        previous = embedded
        state = embedded
        layers = cross_down.shape[0]
        for layer in range(layers):
            if layer:
                term = jnp.dot(state, cross_down[layer], preferred_element_type=jnp.float32)
                term = term.astype(jnp.bfloat16)
                if c == len(PLAN) - 2:
                    previous = term
            low = sum_over(term, "mp")
            if layer < layers - 1:
                high = (
                    jnp.dot(low, cross_up[layer], preferred_element_type=jnp.float32)
                    + cross_bias[layer][None, :]
                )
                state = (
                    embedded.astype(jnp.float32) * high + state.astype(jnp.float32)
                ).astype(jnp.bfloat16)
            else:
                if finish is not None and not final:
                    out = finish(out)
                finish = functools.partial(
                    last,
                    low,
                    cross_up[layer],
                    cross_bias[layer],
                    embedded,
                    state,
                    begin,
                    (groups, share, width),
                )
    out = finish(out)
    return out.reshape(examples, width)


def solution(mesh):
    return jax.shard_map(
        stages,
        mesh=mesh,
        in_specs=(
            P("batch", None),
            P(),
            P("batch", None, None),
            P(None, "mp", None),
            P(None, None, "mp"),
            P(None, "mp"),
        ),
        out_specs=P("batch", "mp"),
        check_vma=False,
    )
```
